32 devices in a mesh: prefix: 4 (over z), resp: 8 (over y, x, core).
Axes of the slice: x: 2, y: 2, z: 4, core: 2. Of those that a mesh axis runs over, the one named last changes fastest.
Arguments:
- prompt_kv: bfloat16 [2, 128, 512], P(None, 'prefix'), may hold values from -6 to 6
- response_queries: bfloat16 [64, 128, 1792], P(('prefix', 'resp')), may hold values from -300 to 300
- resp_kv: bfloat16 [64, 128, 512], P(('prefix', 'resp')), may hold values from -6 to 6
- readout: bfloat16 [64, 128, 1792], P(('prefix', 'resp')), may hold values from -3 to 3
- slot_response: int32 [64], P(('prefix', 'resp')), may hold values from 0 to 63, each once
- lengths: int32 [64], replicated, may hold values from 32 to 128
- pair_prompt: int32 [32], replicated, may hold values from 0 to 1
- ref_margin: float32 [32], replicated, may hold values from -60 to 60
Outputs:
- margins: float32 [32], replicated
- grad_q: bfloat16 [64, 128, 1792], P(('prefix', 'resp'))
- grad_resp_kv: bfloat16 [64, 128, 512], P(('prefix', 'resp'))
- grad_prompt_kv: bfloat16 [2, 128, 512], P(None, 'prefix')
The draws below stay inside these ranges and needn't reach their ends.
Inputs may be any that keep to these rules, and one draw needn't show every extreme that they name: `slot_response`: each response appears in exactly one slot; response 2 k is the chosen and 2 k + 1 the rejected response of pair k.
All inputs are finite; a program needn't handle non-finite values.
Results may differ from the reference program's by a relative error of at most 0.015.
Values may be sent and summed in bfloat16 or wider, within the bound.
A program may use at most 64 MiB of HBM per device.

```python
import jax
import jax.numpy as jnp
from jax import lax

QUERY_HEADS = 14
KEY_VALUE_HEADS = 2
HEAD_SIZE = 128
RESPONSE_TOKENS = 128
PROMPT_COUNT = 2
PROMPT_TOKENS = 128
RESPONSE_COUNT = 64
PAIRS = 32
QW = 1792
KVW = 256


def draw_response_queries(key, part):
    offset_start = jnp.clip(jax.random.normal(jax.random.fold_in(key, 11), (RESPONSE_COUNT, RESPONSE_TOKENS, QUERY_HEADS, HEAD_SIZE), jnp.float32), -6.0, 6.0)
    return offset_start.reshape(RESPONSE_COUNT, RESPONSE_TOKENS, QUERY_HEADS * HEAD_SIZE).astype(jnp.bfloat16)


def draw_prompt_kv(key, part):
    offset_start = jnp.clip(jax.random.normal(jax.random.fold_in(key, 23), (PROMPT_COUNT, PROMPT_TOKENS, 2 * KEY_VALUE_HEADS * HEAD_SIZE), jnp.float32), -6.0, 6.0)
    return offset_start.astype(jnp.bfloat16)


def plant(drawn, stream_key, least, largest):
    longest = drawn.shape.index(max(drawn.shape))
    spots = []
    for shift in (0, 1):
        where = [jax.random.randint(jax.random.fold_in(stream_key, axis), (), 0, length) for axis, length in enumerate(drawn.shape)]
        where[longest] = (where[longest] + shift) % drawn.shape[longest]
        spots.append(tuple(where))
    return drawn.at[spots[0]].set(least).at[spots[1]].set(largest)


def shard_levels(rng, extent, cuts, low, largest):
    gain = 1.0
    for axis_at, blocks in cuts:
        heights = jax.random.uniform(jax.random.fold_in(jax.random.fold_in(rng, 6), axis_at), (blocks,), jnp.float32, low / len(cuts), largest / len(cuts))
        gain = gain * jnp.repeat(jnp.exp(heights), extent[axis_at] // blocks).reshape((-1,) + (1,) * (len(extent) - 1 - axis_at))
    return gain


def noise(key, extent, width, reach, cuts=(), kind=jnp.bfloat16):
    values = width * jax.random.normal(key, extent, jnp.float32)
    if cuts:
        values = values * shard_levels(key, extent, cuts, -0.22, 0.18)
    return jnp.clip(values, -reach, reach).astype(kind)


def setup_inputs(seed: int = 0) -> dict:
    key_of = jax.random.split(jax.random.key(seed), 9)
    prompt_kv = draw_prompt_kv(jax.random.fold_in(key_of[8], 71), 0)
    response_queries = draw_response_queries(jax.random.fold_in(key_of[8], 71), 0)
    resp_kv = noise(key_of[2], (RESPONSE_COUNT, RESPONSE_TOKENS, 2 * KVW), 1.0, 6.0, ((0, 32),))
    readout = noise(key_of[3], (RESPONSE_COUNT, RESPONSE_TOKENS, QW), 0.5, 3.0, ((0, 32),))
    slot_response = jax.random.permutation(key_of[4], RESPONSE_COUNT).astype(jnp.int32)
    lengths = plant(jax.random.randint(key_of[5], (RESPONSE_COUNT,), RESPONSE_TOKENS // 4, RESPONSE_TOKENS + 1), jax.random.fold_in(key_of[5], 1), RESPONSE_TOKENS // 4, RESPONSE_TOKENS).astype(jnp.int32)
    pair_prompt = plant(jax.random.randint(key_of[6], (PAIRS,), 0, PROMPT_COUNT), jax.random.fold_in(key_of[6], 1), 0, PROMPT_COUNT - 1).astype(jnp.int32)
    ref_margin = noise(key_of[7], (PAIRS,), 10.0, 60.0, (), jnp.float32)
    return {"prompt_kv": prompt_kv, "response_queries": response_queries, "resp_kv": resp_kv, "readout": readout, "slot_response": slot_response, "lengths": lengths, "pair_prompt": pair_prompt, "ref_margin": ref_margin}


margin_beta = 0.1
loss_scale = 256.0
highest = lax.Precision.HIGHEST


def inner_product(form, left, right):
    return jnp.einsum(form, left.astype(jnp.float32), right.astype(jnp.float32), precision=highest)


def unpack(packed_rows):
    row_block = packed_rows.shape[0]
    key_rows = packed_rows[:, :KEY_VALUE_HEADS * HEAD_SIZE].reshape(row_block, KEY_VALUE_HEADS, HEAD_SIZE)
    value_rows = packed_rows[:, KEY_VALUE_HEADS * HEAD_SIZE:].reshape(row_block, KEY_VALUE_HEADS, HEAD_SIZE)
    return key_rows, value_rows


def forward_pieces(query_rows, prompt_packed, own_packed):
    prompt_keys, prompt_values = unpack(prompt_packed)
    own_keys, own_values = unpack(own_packed)
    positions = jnp.arange(RESPONSE_TOKENS)
    causal = positions[None, :] <= positions[:, None]
    scale_factor = HEAD_SIZE ** -0.5
    prompt_scores = inner_product("tgjd,kgd->gjtk", query_rows, prompt_keys) * scale_factor
    own_scores = inner_product("tgjd,kgd->gjtk", query_rows, own_keys) * scale_factor
    own_scores = jnp.where(causal, own_scores, -jnp.inf)
    row_max = jnp.maximum(jnp.max(prompt_scores, -1, keepdims=True), jnp.max(own_scores, -1, keepdims=True))
    prompt_exp = jnp.exp(prompt_scores - row_max)
    own_exp = jnp.exp(own_scores - row_max)
    total = jnp.sum(prompt_exp, -1, keepdims=True) + jnp.sum(own_exp, -1, keepdims=True)
    prefix_probabilities = (prompt_exp / total).astype(jnp.bfloat16)
    self_probabilities = (own_exp / total).astype(jnp.bfloat16)
    attended = inner_product("gjtk,kgd->tgjd", prefix_probabilities, prompt_values) + inner_product("gjtk,kgd->tgjd", self_probabilities, own_values)
    return prompt_keys, prompt_values, own_keys, own_values, prefix_probabilities, self_probabilities, attended


def reference(prompt_kv, response_queries, resp_kv, readout, slot_response, lengths, pair_prompt, ref_margin):
    query_groups = QUERY_HEADS // KEY_VALUE_HEADS
    scale_factor = HEAD_SIZE ** -0.5
    query_rows_total = response_queries.reshape(RESPONSE_COUNT, RESPONSE_TOKENS, KEY_VALUE_HEADS, query_groups, HEAD_SIZE)
    output_rows_total = readout.reshape(RESPONSE_COUNT, RESPONSE_TOKENS, KEY_VALUE_HEADS, query_groups, HEAD_SIZE)
    pair_of_slot = (slot_response // 2).astype(jnp.int32)
    sign_of_slot = 1.0 - 2.0 * (slot_response % 2).astype(jnp.float32)
    length_of_slot = lengths[slot_response]
    prompt_of_slot = pair_prompt[pair_of_slot].astype(jnp.int32)

    def slot_logp(items):
        query_rows, own_packed, output_rows, prompt, length = items
        prompt_packed = lax.dynamic_index_in_dim(prompt_kv, prompt, 0, keepdims=False)
        attended = forward_pieces(query_rows, prompt_packed, own_packed)[-1]
        valid = (jnp.arange(RESPONSE_TOKENS) < length).astype(jnp.float32)
        token_logp = jnp.sum(attended * output_rows.astype(jnp.float32), axis=(1, 2, 3)) * valid
        return jnp.sum(token_logp)

    slot_sums = lax.map(slot_logp, (query_rows_total, resp_kv, output_rows_total, prompt_of_slot, length_of_slot))
    pair_sums = jnp.zeros((PAIRS,), jnp.float32).at[pair_of_slot].add(sign_of_slot * slot_sums)
    margins = margin_beta * (pair_sums - ref_margin)
    weights = -loss_scale * margin_beta * jax.nn.sigmoid(-margins)
    coefficient_of_slot = weights[pair_of_slot] * sign_of_slot

    def slot_backward(partial_value, items):
        query_rows, own_packed, output_rows, prompt, length, coefficient = items
        prompt_packed = lax.dynamic_index_in_dim(prompt_kv, prompt, 0, keepdims=False)
        prompt_keys, prompt_values, own_keys, own_values, prefix_probabilities, self_probabilities, attended = forward_pieces(query_rows, prompt_packed, own_packed)
        valid = (jnp.arange(RESPONSE_TOKENS) < length).astype(jnp.float32)
        output_gradient = (coefficient * output_rows.astype(jnp.float32) * valid[:, None, None, None]).astype(jnp.bfloat16)
        prompt_dprobs = inner_product("tgjd,kgd->gjtk", output_gradient, prompt_values)
        own_dprobs = inner_product("tgjd,kgd->gjtk", output_gradient, own_values)
        delta = jnp.transpose(jnp.sum(output_gradient.astype(jnp.float32) * attended, -1), (1, 2, 0))[..., None]
        prefix_score_gradient = (prefix_probabilities.astype(jnp.float32) * (prompt_dprobs - delta) * scale_factor).astype(jnp.bfloat16)
        self_score_gradient = (self_probabilities.astype(jnp.float32) * (own_dprobs - delta) * scale_factor).astype(jnp.bfloat16)
        grad_queries = inner_product("gjtk,kgd->tgjd", prefix_score_gradient, prompt_keys) + inner_product("gjtk,kgd->tgjd", self_score_gradient, own_keys)
        prompt_grad = jnp.concatenate([
            inner_product("hybi,bhyu->ihu", prefix_score_gradient, query_rows).reshape(PROMPT_TOKENS, KEY_VALUE_HEADS * HEAD_SIZE),
            inner_product("hybi,bhyu->ihu", prefix_probabilities, output_gradient).reshape(PROMPT_TOKENS, KEY_VALUE_HEADS * HEAD_SIZE)], axis=-1)
        own_grad = jnp.concatenate([
            inner_product("hybi,bhyu->ihu", self_score_gradient, query_rows).reshape(RESPONSE_TOKENS, KEY_VALUE_HEADS * HEAD_SIZE),
            inner_product("hybi,bhyu->ihu", self_probabilities, output_gradient).reshape(RESPONSE_TOKENS, KEY_VALUE_HEADS * HEAD_SIZE)], axis=-1)
        selector = (jnp.arange(PROMPT_COUNT) == prompt)[:, None, None]
        partial_value = partial_value + jnp.where(selector, prompt_grad[None], 0.0)
        return partial_value, (grad_queries.reshape(RESPONSE_TOKENS, QUERY_HEADS * HEAD_SIZE).astype(jnp.bfloat16), own_grad.astype(jnp.bfloat16))

    begin_offset = jnp.zeros((PROMPT_COUNT, PROMPT_TOKENS, 2 * KEY_VALUE_HEADS * HEAD_SIZE), jnp.float32)
    partial_value, outputs = lax.scan(slot_backward, begin_offset, (query_rows_total, resp_kv, output_rows_total, prompt_of_slot, length_of_slot, coefficient_of_slot))
    grad_q, grad_resp_kv = outputs
    return margins, grad_q, grad_resp_kv, partial_value.astype(jnp.bfloat16)
```

```python
import functools

import jax
import jax.numpy as jnp
from jax import lax
from jax.experimental import pallas as pl
from jax.experimental.pallas import tpu as pltpu
from jax.sharding import PartitionSpec as P

QUERY_HEADS = 14
KEY_VALUE_HEADS = 2
HEAD_SIZE = 128
LANES = 128
ROWS = 16

margin_beta = 0.1
loss_scale = 256.0
MESH = pl.DeviceIdType.MESH
F32 = jnp.float32
BF16 = jnp.bfloat16


def dot_nt(a, b):
    return lax.dot_general(a, b, (((1,), (1,)), ((), ())), preferred_element_type=F32)


def dot_nn(a, b):
    return lax.dot_general(a, b, (((1,), (0,)), ((), ())), preferred_element_type=F32)


def kernel(
    np_, nr,
    prompt_hbm, q_hbm, kv_hbm, ro_hbm, slot_ref, len_ref, pp_ref, ppv_ref, rm_ref,
    margins_out, gq_out, gkv_out, gp_out,
    full, qv, kvv, rov, ds_s, p_s, gq_s, gkv_s, g_send, g_all, info_all, fin_all, lanes_s,
    in_sem, pk_ssem, pk_rsem, g_ssem, g_rsem, i_ssem, i_rsem, f_ssem, f_rsem,
):
    n = np_ * nr
    prompts, local, width = prompt_hbm.shape
    slots, tokens, _ = q_hbm.shape
    pairs = rm_ref.shape[1]
    pl_w = info_all.shape[2]
    groups = QUERY_HEADS // KEY_VALUE_HEADS
    col_tiles = width // LANES
    tiles = (local // ROWS) * col_tiles
    total_len = full.shape[1]
    scale = HEAD_SIZE ** (-0.5)
    p = lax.axis_index("prefix")
    r = lax.axis_index("resp")
    me = p * nr + r

    def at_offset(k):
        other = lax.rem(me + k, n)
        return other, other // nr, lax.rem(other, nr)

    own_rows = full.at[:, pl.ds(pl.multiple_of(p * local, local), local), :]
    loads = [
        pltpu.make_async_copy(prompt_hbm, own_rows, in_sem.at[0]),
        pltpu.make_async_copy(q_hbm, qv, in_sem.at[1]),
        pltpu.make_async_copy(kv_hbm, kvv, in_sem.at[2]),
        pltpu.make_async_copy(ro_hbm, rov, in_sem.at[3]),
    ]
    for c in loads:
        c.start()

    barrier = pltpu.get_barrier_semaphore()

    def greet(k, carry):
        _, op, orr = at_offset(k)
        pl.semaphore_signal(barrier, inc=1, device_id=(op, orr), device_id_type=MESH)
        return carry

    lax.fori_loop(1, n, greet, 0)

    lanes_s[...] = jnp.zeros_like(lanes_s)
    lanes_s[0:1, 0:pairs] = rm_ref[...]
    lanes_s[1:2, 0:pairs] = ppv_ref[...].astype(F32)
    info_all[me] = jnp.zeros((info_all.shape[1], pl_w), F32)

    loads[0].wait()
    pl.semaphore_wait(barrier, n - 1)

    def prompt_copy(owner, to):
        rows = full.at[:, pl.ds(pl.multiple_of(owner * local, local), local), :]
        return pltpu.make_async_remote_copy(
            src_ref=rows, dst_ref=rows, send_sem=pk_ssem.at[to], recv_sem=pk_rsem.at[owner],
            device_id=(to, r), device_id_type=MESH,
        )

    others = [lax.rem(p + k, np_) for k in range(1, np_)]
    for o in others:
        prompt_copy(p, o).start()
    for c in loads[1:]:
        c.wait()
    for o in others:
        prompt_copy(o, p).wait_recv()

    causal = (
        lax.broadcasted_iota(jnp.int32, (tokens, tokens), 0)
        <= lax.broadcasted_iota(jnp.int32, (tokens, tokens), 1)
    )
    lane_t = lax.broadcasted_iota(jnp.int32, (1, tokens), 1)
    lane_k = lax.broadcasted_iota(jnp.int32, (1, pl_w), 1)

    def one_slot(s, carry):
        response = slot_ref[s]
        pair = lax.shift_right_logical(response, 1)
        sign = 1.0 - 2.0 * lax.bitwise_and(response, 1).astype(F32)
        valid = (lane_t < len_ref[response]).astype(F32)
        a = pp_ref[pair]
        logp = jnp.zeros((1, tokens), F32)
        for g in range(KEY_VALUE_HEADS):
            kc = slice(g * HEAD_SIZE, (g + 1) * HEAD_SIZE)
            vc = slice((KEY_VALUE_HEADS + g) * HEAD_SIZE, (KEY_VALUE_HEADS + g + 1) * HEAD_SIZE)
            keys = jnp.concatenate([full[a, :, kc], kvv[s, :, kc]], axis=0)
            values = jnp.concatenate([full[a, :, vc], kvv[s, :, vc]], axis=0)
            for j in range(groups):
                h = g * groups + j
                hc = slice(h * HEAD_SIZE, (h + 1) * HEAD_SIZE)
                jc = slice(j * tokens, (j + 1) * tokens)
                sc = dot_nt(keys, qv[s, :, hc])
                dp = dot_nt(values, rov[s, :, hc])
                sp = sc[:total_len]
                so = jnp.where(causal, sc[total_len:], -jnp.inf)
                top = jnp.maximum(
                    jnp.max(sp, axis=0, keepdims=True), jnp.max(so, axis=0, keepdims=True)
                )
                sc = jnp.concatenate([sp, so], axis=0)
                e = jnp.exp((sc - top) * scale)
                inv = valid / jnp.sum(e, axis=0, keepdims=True)
                pb = (e * inv).astype(BF16)
                pf = pb.astype(F32)
                delta = jnp.sum(pf * dp, axis=0, keepdims=True)
                logp = logp + delta
                p_s[:, jc] = pb
                ds_s[:, jc] = (pf * (dp - delta)).astype(BF16)
            gqt = dot_nn(keys.T, ds_s[...])
            for j in range(groups):
                h = g * groups + j
                hc = slice(h * HEAD_SIZE, (h + 1) * HEAD_SIZE)
                gq_s[s, :, hc] = gqt[:, j * tokens:(j + 1) * tokens].T
            heads = range(g * groups, (g + 1) * groups)
            qs = jnp.concatenate([qv[s, :, h * HEAD_SIZE:(h + 1) * HEAD_SIZE] for h in heads], axis=0)
            rs = jnp.concatenate([rov[s, :, h * HEAD_SIZE:(h + 1) * HEAD_SIZE] for h in heads], axis=0)
            gk = dot_nn(ds_s[...], qs) * scale
            gv = dot_nn(p_s[...], rs)
            gkv_s[s, :, kc] = gk[total_len:]
            gkv_s[s, :, vc] = gv[total_len:]
            for o in range(np_):
                for i in range(local // ROWS):
                    rows = slice(o * local + i * ROWS, o * local + (i + 1) * ROWS)
                    at = o * tiles + i * col_tiles
                    g_send[at + g, s] = gk[rows].astype(BF16)
                    g_send[at + KEY_VALUE_HEADS + g, s] = gv[rows].astype(BF16)
        hot = jnp.where(lane_k == pair, sign, 0.0)
        info_all[me, pl.ds(s, 1), :] = hot
        info_all[me, pl.ds(slots + s, 1), :] = hot * jnp.sum(logp, axis=1, keepdims=True)
        return carry

    lax.fori_loop(0, slots, one_slot, 0)

    def info_copy(sender, other, op, orr):
        return pltpu.make_async_remote_copy(
            src_ref=info_all.at[sender], dst_ref=info_all.at[sender],
            send_sem=i_ssem.at[other], recv_sem=i_rsem.at[sender],
            device_id=(op, orr), device_id_type=MESH,
        )

    def tile_copy(sender, other, op, orr):
        return pltpu.make_async_remote_copy(
            src_ref=g_send.at[op * tiles + orr], dst_ref=g_all.at[sender],
            send_sem=g_ssem.at[other], recv_sem=g_rsem.at[sender],
            device_id=(op, orr), device_id_type=MESH,
        )

    def when_owner(rank, f):
        if nr == tiles:
            f()
        else:
            pl.when(rank < tiles)(f)

    def send(k, carry):
        other, op, orr = at_offset(k)
        info_copy(me, other, op, orr).start()
        when_owner(orr, lambda: tile_copy(me, other, op, orr).start())
        return carry

    lax.fori_loop(1, n, send, 0)

    def take_own():
        g_all[me] = g_send[p * tiles + r]

    when_owner(r, take_own)

    def info_wait(k, carry):
        other, op, orr = at_offset(k)
        info_copy(other, other, op, orr).wait_recv()
        return carry

    lax.fori_loop(1, n, info_wait, 0)

    chunk = min(n, 32)

    def add_info(c, acc):
        return acc + jnp.sum(info_all[pl.ds(c * chunk, chunk)], axis=0)

    sums = lax.fori_loop(0, n // chunk, add_info, jnp.zeros((info_all.shape[1], pl_w), F32))
    pair_sums = jnp.sum(sums[slots:2 * slots], axis=0, keepdims=True)
    margins = margin_beta * (pair_sums - lanes_s[0:1, :])
    margins_out[...] = margins[:, 0:pairs]
    weights = -loss_scale * margin_beta * jax.nn.sigmoid(-margins)
    weights = jnp.where(lane_k < pairs, weights, 0.0)

    def finish_tile():
        def tile_wait(k, carry):
            other, op, orr = at_offset(k)
            pltpu.make_async_remote_copy(
                src_ref=g_send.at[0], dst_ref=g_all.at[other],
                send_sem=g_ssem.at[other], recv_sem=g_rsem.at[other],
                device_id=(op, orr), device_id_type=MESH,
            ).wait_recv()
            return carry

        lax.fori_loop(1, n, tile_wait, 0)

        def add_tiles(c, acc):
            x = info_all[pl.ds(c * chunk, chunk)]
            acc = list(acc)
            for a in range(prompts):
                wa = jnp.where(lanes_s[1:2, :] == float(a), weights, 0.0)
                ca = jnp.sum(x * wa[None], axis=-1, keepdims=True)
                for d in range(chunk):
                    for s in range(slots):
                        acc[a] = acc[a] + ca[d, s:s + 1, :] * g_all[c * chunk + d, s].astype(F32)
            return tuple(acc)

        zero = tuple(jnp.zeros((ROWS, LANES), F32) for _ in range(prompts))
        acc = lax.fori_loop(0, n // chunk, add_tiles, zero)
        for a in range(prompts):
            fin_all[r, a] = acc[a].astype(BF16)

        def fin_send(k, carry):
            orr = lax.rem(r + k, nr)
            pltpu.make_async_remote_copy(
                src_ref=fin_all.at[r], dst_ref=fin_all.at[r],
                send_sem=f_ssem.at[orr], recv_sem=f_rsem.at[r],
                device_id=(p, orr), device_id_type=MESH,
            ).start()
            return carry

        lax.fori_loop(1, nr, fin_send, 0)

    when_owner(r, finish_tile)

    for s in range(slots):
        coef = jnp.sum(info_all[me, s:s + 1, :] * weights, axis=1, keepdims=True)
        gq_out[s] = (gq_s[s] * (coef * scale)).astype(BF16)
        gkv_out[s] = (gkv_s[s] * coef).astype(BF16)

    def fin_copy(sender, other):
        return pltpu.make_async_remote_copy(
            src_ref=fin_all.at[sender], dst_ref=fin_all.at[sender],
            send_sem=f_ssem.at[other], recv_sem=f_rsem.at[sender],
            device_id=(p, other), device_id_type=MESH,
        )

    def fin_wait(k, carry):
        other = lax.rem(r + k, nr)
        when_owner(other, lambda: fin_copy(other, other).wait_recv())
        return carry

    lax.fori_loop(1, nr, fin_wait, 0)
    for t in range(tiles):
        i, j = divmod(t, col_tiles)
        for a in range(prompts):
            gp_out[a, i * ROWS:(i + 1) * ROWS, j * LANES:(j + 1) * LANES] = fin_all[t, a]

    def drain(k, carry):
        other, op, orr = at_offset(k)
        info_copy(me, other, op, orr).wait_send()
        when_owner(orr, lambda: tile_copy(me, other, op, orr).wait_send())
        return carry

    lax.fori_loop(1, n, drain, 0)
    for o in others:
        prompt_copy(p, o).wait_send()

    def drain_fin():
        def one(k, carry):
            fin_copy(r, lax.rem(r + k, nr)).wait_send()
            return carry

        lax.fori_loop(1, nr, one, 0)

    when_owner(r, drain_fin)


def on_device(np_, nr, prompt_kv, response_queries, resp_kv, readout, slot_response, lengths, pair_prompt, ref_margin):
    n = np_ * nr
    prompts, local, width = prompt_kv.shape
    slots, tokens, qw = response_queries.shape
    pairs = ref_margin.shape[0]
    pl_w = -(-pairs // LANES) * LANES
    total_len = local * np_
    groups = QUERY_HEADS // KEY_VALUE_HEADS
    tiles = (local // ROWS) * (width // LANES)
    assert nr >= tiles
    info_rows = -(-2 * slots // 8) * 8
    keys = total_len + tokens
    any_space = pl.BlockSpec(memory_space=pl.ANY)
    vmem = pl.BlockSpec(memory_space=pltpu.VMEM)
    smem = pl.BlockSpec(memory_space=pltpu.SMEM)
    dma = pltpu.SemaphoreType.DMA
    margins, gq, gkv, gp = pl.pallas_call(
        functools.partial(kernel, np_, nr),
        name="dpo_attention",
        out_shape=(
            jax.ShapeDtypeStruct((1, pairs), F32),
            jax.ShapeDtypeStruct(response_queries.shape, BF16),
            jax.ShapeDtypeStruct(resp_kv.shape, BF16),
            jax.ShapeDtypeStruct(prompt_kv.shape, BF16),
        ),
        in_specs=[any_space] * 4 + [smem] * 3 + [vmem] * 2,
        out_specs=(vmem,) * 4,
        scratch_shapes=[
            pltpu.VMEM((prompts, total_len, width), BF16),
            pltpu.VMEM((slots, tokens, qw), BF16),
            pltpu.VMEM((slots, tokens, width), BF16),
            pltpu.VMEM((slots, tokens, qw), BF16),
            pltpu.VMEM((keys, groups * tokens), BF16),
            pltpu.VMEM((keys, groups * tokens), BF16),
            pltpu.VMEM((slots, tokens, qw), F32),
            pltpu.VMEM((slots, tokens, width), F32),
            pltpu.VMEM((np_ * tiles, slots, ROWS, LANES), BF16),
            pltpu.VMEM((n, slots, ROWS, LANES), BF16),
            pltpu.VMEM((n, info_rows, pl_w), F32),
            pltpu.VMEM((tiles, prompts, ROWS, LANES), BF16),
            pltpu.VMEM((8, pl_w), F32),
            dma((4,)),
            dma((np_,)), dma((np_,)),
            dma((n,)), dma((n,)),
            dma((n,)), dma((n,)),
            dma((nr,)), dma((nr,)),
        ],
        compiler_params=pltpu.CompilerParams(collective_id=0, has_side_effects=True),
    )(
        prompt_kv, response_queries, resp_kv, readout, slot_response, lengths, pair_prompt,
        pair_prompt.reshape(1, pairs), ref_margin.reshape(1, pairs),
    )
    return margins.reshape(pairs), gq, gkv, gp


def solution(mesh):
    both = ("prefix", "resp")
    in_specs = (
        P(None, "prefix", None),
        P(both, None, None),
        P(both, None, None),
        P(both, None, None),
        P(both),
        P(),
        P(),
        P(),
    )
    out_specs = (
        P(),
        P(both, None, None),
        P(both, None, None),
        P(None, "prefix", None),
    )
    return jax.shard_map(
        functools.partial(on_device, mesh.shape["prefix"], mesh.shape["resp"]),
        mesh=mesh, in_specs=in_specs, out_specs=out_specs, check_vma=False,
    )
```

```python
import functools

import jax
import jax.numpy as jnp
from jax import lax
from jax.experimental import pallas as pl
from jax.experimental.pallas import tpu as pltpu
from jax.sharding import PartitionSpec as P

QUERY_HEADS = 14
KEY_VALUE_HEADS = 2
HEAD_SIZE = 128
LANES = 128
ROWS = 16

margin_beta = 0.1
loss_scale = 256.0
MESH = pl.DeviceIdType.MESH
F32 = jnp.float32
BF16 = jnp.bfloat16


def dot_nt(a, b):
    return lax.dot_general(a, b, (((1,), (1,)), ((), ())), preferred_element_type=F32)


def dot_nn(a, b):
    return lax.dot_general(a, b, (((1,), (0,)), ((), ())), preferred_element_type=F32)


def kernel(
    np_, nr,
    prompt_hbm, q_hbm, kv_hbm, ro_hbm, slot_ref, len_ref, pp_ref, ppv_ref, rm_ref,
    margins_out, gq_s, gkv_s, fin_out, coef_out,
    full, qv, kvv, rov, ds_s, p_s, g_send, g_all, info_all, fin_all, lanes_s,
    in_sem, pk_ssem, pk_rsem, pd_ssem, pd_rsem, g_ssem, g_rsem, i_ssem, i_rsem, f_ssem, f_rsem,
):
    n = np_ * nr
    prompts, local, width = prompt_hbm.shape
    slots, tokens, _ = q_hbm.shape
    pairs = rm_ref.shape[1]
    pl_w = info_all.shape[2]
    groups = QUERY_HEADS // KEY_VALUE_HEADS
    col_tiles = width // LANES
    tiles = (local // ROWS) * col_tiles
    total_len = full.shape[1]
    scale = HEAD_SIZE ** (-0.5)
    p = lax.axis_index("prefix")
    r = lax.axis_index("resp")
    me = p * nr + r

    def at_offset(k):
        other = lax.rem(me + k, n)
        return other, other // nr, lax.rem(other, nr)

    own_rows = full.at[:, pl.ds(pl.multiple_of(p * local, local), local), :]
    loads = [
        pltpu.make_async_copy(prompt_hbm, own_rows, in_sem.at[0]),
        pltpu.make_async_copy(q_hbm, qv, in_sem.at[1]),
        pltpu.make_async_copy(kv_hbm, kvv, in_sem.at[2]),
        pltpu.make_async_copy(ro_hbm, rov, in_sem.at[3]),
    ]
    for c in loads:
        c.start()

    barrier = pltpu.get_barrier_semaphore()

    def greet(k, carry):
        _, op, orr = at_offset(k)
        pl.semaphore_signal(barrier, inc=1, device_id=(op, orr), device_id_type=MESH)
        return carry

    lax.fori_loop(1, n, greet, 0)

    lanes_s[...] = jnp.zeros_like(lanes_s)
    lanes_s[0:1, 0:pairs] = rm_ref[...]
    lanes_s[1:2, 0:pairs] = ppv_ref[...].astype(F32)
    info_all[me] = jnp.zeros((info_all.shape[1], pl_w), F32)

    loads[0].wait()
    pl.semaphore_wait(barrier, n - 1)

    half = lax.rem(r, 2)
    partner = r + 1 - 2 * half
    half_width = width // 2

    def half_of(owner, which):
        rows = pl.ds(pl.multiple_of(owner * local, local), local)
        return full.at[:, rows, pl.ds(pl.multiple_of(which * half_width, half_width), half_width)]

    def prompt_copy(owner, to):
        part = half_of(owner, half)
        return pltpu.make_async_remote_copy(
            src_ref=part, dst_ref=part, send_sem=pk_ssem.at[to], recv_sem=pk_rsem.at[owner],
            device_id=(to, r), device_id_type=MESH,
        )

    def pass_copy(owner, which):
        part = half_of(owner, which)
        return pltpu.make_async_remote_copy(
            src_ref=part, dst_ref=part, send_sem=pd_ssem.at[owner], recv_sem=pd_rsem.at[owner],
            device_id=(p, partner), device_id_type=MESH,
        )

    others = [lax.rem(p + k, np_) for k in range(1, np_)]
    for o in others:
        prompt_copy(p, o).start()
    for c in loads[1:]:
        c.wait()
    for o in others:
        prompt_copy(o, p).wait_recv()
        pass_copy(o, half).start()
    for o in others:
        pass_copy(o, 1 - half).wait_recv()

    causal = (
        lax.broadcasted_iota(jnp.int32, (tokens, tokens), 0)
        <= lax.broadcasted_iota(jnp.int32, (tokens, tokens), 1)
    )
    lane_t = lax.broadcasted_iota(jnp.int32, (1, tokens), 1)
    lane_k = lax.broadcasted_iota(jnp.int32, (1, pl_w), 1)

    def info_copy(sender, other, op, orr):
        return pltpu.make_async_remote_copy(
            src_ref=info_all.at[sender], dst_ref=info_all.at[sender],
            send_sem=i_ssem.at[other], recv_sem=i_rsem.at[sender],
            device_id=(op, orr), device_id_type=MESH,
        )

    def tile_copy(s, sender, other, op, orr):
        return pltpu.make_async_remote_copy(
            src_ref=g_send.at[s, op * tiles + orr], dst_ref=g_all.at[sender, s],
            send_sem=g_ssem.at[s, other], recv_sem=g_rsem.at[s, sender],
            device_id=(op, orr), device_id_type=MESH,
        )

    def when_owner(rank, f):
        if nr == tiles:
            f()
        else:
            pl.when(rank < tiles)(f)

    def one_slot(s, carry):
        response = slot_ref[s]
        pair = lax.shift_right_logical(response, 1)
        sign = 1.0 - 2.0 * lax.bitwise_and(response, 1).astype(F32)
        valid = (lane_t < len_ref[response]).astype(F32)
        a = pp_ref[pair]
        logp = jnp.zeros((1, tokens), F32)
        for g in range(KEY_VALUE_HEADS):
            kc = slice(g * HEAD_SIZE, (g + 1) * HEAD_SIZE)
            vc = slice((KEY_VALUE_HEADS + g) * HEAD_SIZE, (KEY_VALUE_HEADS + g + 1) * HEAD_SIZE)
            keys = jnp.concatenate([full[a, :, kc], kvv[s, :, kc]], axis=0)
            values = jnp.concatenate([full[a, :, vc], kvv[s, :, vc]], axis=0)
            for j in range(groups):
                h = g * groups + j
                hc = slice(h * HEAD_SIZE, (h + 1) * HEAD_SIZE)
                jc = slice(j * tokens, (j + 1) * tokens)
                sc = dot_nt(keys, qv[s, :, hc])
                dp = dot_nt(values, rov[s, :, hc])
                sp = sc[:total_len]
                so = jnp.where(causal, sc[total_len:], -jnp.inf)
                top = jnp.maximum(
                    jnp.max(sp, axis=0, keepdims=True), jnp.max(so, axis=0, keepdims=True)
                )
                sc = jnp.concatenate([sp, so], axis=0)
                e = jnp.exp((sc - top) * scale)
                inv = valid / jnp.sum(e, axis=0, keepdims=True)
                pb = (e * inv).astype(BF16)
                pf = pb.astype(F32)
                delta = jnp.sum(pf * dp, axis=0, keepdims=True)
                logp = logp + delta
                p_s[:, jc] = pb
                ds_s[:, jc] = (pf * (dp - delta)).astype(BF16)
            gqt = dot_nn(keys.T, ds_s[...])
            for j in range(groups):
                h = g * groups + j
                hc = slice(h * HEAD_SIZE, (h + 1) * HEAD_SIZE)
                gq_s[s, :, hc] = gqt[:, j * tokens:(j + 1) * tokens].T
            heads = range(g * groups, (g + 1) * groups)
            qs = jnp.concatenate([qv[s, :, h * HEAD_SIZE:(h + 1) * HEAD_SIZE] for h in heads], axis=0)
            rs = jnp.concatenate([rov[s, :, h * HEAD_SIZE:(h + 1) * HEAD_SIZE] for h in heads], axis=0)
            gk = dot_nn(ds_s[...], qs) * scale
            gv = dot_nn(p_s[...], rs)
            gkv_s[s, :, kc] = gk[total_len:]
            gkv_s[s, :, vc] = gv[total_len:]
            for o in range(np_):
                for i in range(local // ROWS):
                    rows = slice(o * local + i * ROWS, o * local + (i + 1) * ROWS)
                    at = o * tiles + i * col_tiles
                    g_send[s, at + g] = gk[rows].astype(BF16)
                    g_send[s, at + KEY_VALUE_HEADS + g] = gv[rows].astype(BF16)
        hot = jnp.where(lane_k == pair, sign, 0.0)
        info_all[me, pl.ds(s, 1), :] = hot
        info_all[me, pl.ds(slots + s, 1), :] = hot * jnp.sum(logp, axis=1, keepdims=True)

        def send_tile(k, c):
            other, op, orr = at_offset(k)
            when_owner(orr, lambda: tile_copy(s, me, other, op, orr).start())
            return c

        lax.fori_loop(1, n, send_tile, 0)
        return carry

    lax.fori_loop(0, slots, one_slot, 0)

    def send(k, carry):
        other, op, orr = at_offset(k)
        info_copy(me, other, op, orr).start()
        return carry

    lax.fori_loop(1, n, send, 0)

    def take_own():
        for s in range(slots):
            g_all[me, s] = g_send[s, p * tiles + r]

    when_owner(r, take_own)

    def info_wait(k, carry):
        other, op, orr = at_offset(k)
        info_copy(other, other, op, orr).wait_recv()
        return carry

    lax.fori_loop(1, n, info_wait, 0)

    chunk = min(n, 32)

    def add_info(c, acc):
        return acc + jnp.sum(info_all[pl.ds(c * chunk, chunk)], axis=0)

    sums = lax.fori_loop(0, n // chunk, add_info, jnp.zeros((info_all.shape[1], pl_w), F32))
    pair_sums = jnp.sum(sums[slots:2 * slots], axis=0, keepdims=True)
    margins = margin_beta * (pair_sums - lanes_s[0:1, :])
    margins_out[...] = margins[:, 0:pairs]
    weights = -loss_scale * margin_beta * jax.nn.sigmoid(-margins)
    weights = jnp.where(lane_k < pairs, weights, 0.0)
    for s in range(slots):
        coef = jnp.sum(info_all[me, s:s + 1, :] * weights, axis=1, keepdims=True)
        coef_out[s:s + 1, :] = jnp.broadcast_to(coef, (1, LANES))

    def finish_tile():
        def tile_wait(k, carry):
            other, op, orr = at_offset(k)
            for s in range(slots):
                pltpu.make_async_remote_copy(
                    src_ref=g_send.at[s, 0], dst_ref=g_all.at[other, s],
                    send_sem=g_ssem.at[s, other], recv_sem=g_rsem.at[s, other],
                    device_id=(op, orr), device_id_type=MESH,
                ).wait_recv()
            return carry

        lax.fori_loop(1, n, tile_wait, 0)

        def add_tiles(c, acc):
            x = info_all[pl.ds(c * chunk, chunk)]
            acc = list(acc)
            for a in range(prompts):
                wa = jnp.where(lanes_s[1:2, :] == float(a), weights, 0.0)
                ca = jnp.sum(x * wa[None], axis=-1, keepdims=True)
                for d in range(chunk):
                    for s in range(slots):
                        acc[a] = acc[a] + ca[d, s:s + 1, :] * g_all[c * chunk + d, s].astype(F32)
            return tuple(acc)

        zero = tuple(jnp.zeros((ROWS, LANES), F32) for _ in range(prompts))
        acc = lax.fori_loop(0, n // chunk, add_tiles, zero)
        for a in range(prompts):
            fin_all[r, a] = acc[a].astype(BF16)

        def fin_send(k, carry):
            orr = lax.rem(r + k, nr)
            pltpu.make_async_remote_copy(
                src_ref=fin_all.at[r], dst_ref=fin_all.at[r],
                send_sem=f_ssem.at[orr], recv_sem=f_rsem.at[r],
                device_id=(p, orr), device_id_type=MESH,
            ).start()
            return carry

        lax.fori_loop(1, nr, fin_send, 0)

    when_owner(r, finish_tile)

    def fin_copy(sender, other):
        return pltpu.make_async_remote_copy(
            src_ref=fin_all.at[sender], dst_ref=fin_all.at[sender],
            send_sem=f_ssem.at[other], recv_sem=f_rsem.at[sender],
            device_id=(p, other), device_id_type=MESH,
        )

    def fin_wait(k, carry):
        other = lax.rem(r + k, nr)
        when_owner(other, lambda: fin_copy(other, other).wait_recv())
        return carry

    lax.fori_loop(1, nr, fin_wait, 0)
    fin_out[...] = fin_all[...]

    def drain(k, carry):
        other, op, orr = at_offset(k)
        info_copy(me, other, op, orr).wait_send()
        for s in range(slots):
            when_owner(orr, lambda s=s: tile_copy(s, me, other, op, orr).wait_send())
        return carry

    lax.fori_loop(1, n, drain, 0)
    for o in others:
        prompt_copy(p, o).wait_send()
        pass_copy(o, half).wait_send()

    def drain_fin():
        def one(k, carry):
            fin_copy(r, lax.rem(r + k, nr)).wait_send()
            return carry

        lax.fori_loop(1, nr, one, 0)

    when_owner(r, drain_fin)


def finish(margins_ref, gq_ref, gkv_ref, fin_ref, coef_ref, margins_out, gq_out, gkv_out, gp_out, mv, qv, kvv, gpv, sems):
    slots, tokens, qw = gq_ref.shape
    tiles, prompts, _, _ = fin_ref.shape
    width = gkv_ref.shape[2]
    col_tiles = width // LANES
    scale = HEAD_SIZE ** (-0.5)
    pieces = 2
    step = tokens // pieces
    copies = []

    def put(src, dst):
        c = pltpu.make_async_copy(src, dst, sems.at[len(copies)])
        c.start()
        copies.append(c)

    for s in range(slots):
        coef = coef_ref[s:s + 1, 0:1]
        for t in range(pieces):
            rows = slice(t * step, (t + 1) * step)
            qv[s, rows] = (gq_ref[s, rows] * (coef * scale)).astype(BF16)
            put(qv.at[s, rows], gq_out.at[s, rows])
        kvv[s] = (gkv_ref[s] * coef).astype(BF16)
        put(kvv.at[s], gkv_out.at[s])
    for t in range(tiles):
        i, j = divmod(t, col_tiles)
        for a in range(prompts):
            gpv[a, i * ROWS:(i + 1) * ROWS, j * LANES:(j + 1) * LANES] = fin_ref[t, a]
    put(gpv, gp_out)
    mv[...] = margins_ref[...]
    put(mv, margins_out)
    for c in copies:
        c.wait()


def on_device(np_, nr, prompt_kv, response_queries, resp_kv, readout, slot_response, lengths, pair_prompt, ref_margin):
    n = np_ * nr
    prompts, local, width = prompt_kv.shape
    slots, tokens, qw = response_queries.shape
    pairs = ref_margin.shape[0]
    pl_w = -(-pairs // LANES) * LANES
    total_len = local * np_
    groups = QUERY_HEADS // KEY_VALUE_HEADS
    tiles = (local // ROWS) * (width // LANES)
    assert nr >= tiles
    info_rows = 2 * slots
    assert nr % 2 == 0
    keys = total_len + tokens
    any_space = pl.BlockSpec(memory_space=pl.ANY)
    vmem = pl.BlockSpec(memory_space=pltpu.VMEM)
    smem = pl.BlockSpec(memory_space=pltpu.SMEM)
    dma = pltpu.SemaphoreType.DMA
    partial_outs = pl.pallas_call(
        functools.partial(kernel, np_, nr),
        name="dpo_attention",
        out_shape=(
            jax.ShapeDtypeStruct((1, pairs), F32),
            jax.ShapeDtypeStruct(response_queries.shape, F32),
            jax.ShapeDtypeStruct(resp_kv.shape, F32),
            jax.ShapeDtypeStruct((tiles, prompts, ROWS, LANES), BF16),
            jax.ShapeDtypeStruct((8, LANES), F32),
        ),
        in_specs=[any_space] * 4 + [smem] * 3 + [vmem] * 2,
        out_specs=(vmem,) * 5,
        scratch_shapes=[
            pltpu.VMEM((prompts, total_len, width), BF16),
            pltpu.VMEM((slots, tokens, qw), BF16),
            pltpu.VMEM((slots, tokens, width), BF16),
            pltpu.VMEM((slots, tokens, qw), BF16),
            pltpu.VMEM((keys, groups * tokens), BF16),
            pltpu.VMEM((keys, groups * tokens), BF16),
            pltpu.VMEM((slots, np_ * tiles, ROWS, LANES), BF16),
            pltpu.VMEM((n, slots, ROWS, LANES), BF16),
            pltpu.VMEM((n, info_rows, pl_w), F32),
            pltpu.VMEM((tiles, prompts, ROWS, LANES), BF16),
            pltpu.VMEM((8, pl_w), F32),
            dma((4,)),
            dma((np_,)), dma((np_,)), dma((np_,)), dma((np_,)),
            dma((slots, n)), dma((slots, n)),
            dma((n,)), dma((n,)),
            dma((nr,)), dma((nr,)),
        ],
        compiler_params=pltpu.CompilerParams(
            collective_id=0, has_side_effects=True, vmem_limit_bytes=24 * 1024 * 1024
        ),
    )(
        prompt_kv, response_queries, resp_kv, readout, slot_response, lengths, pair_prompt,
        pair_prompt.reshape(1, pairs), ref_margin.reshape(1, pairs),
    )
    margins, gq, gkv, gp = pl.pallas_call(
        finish,
        name="scale_and_store",
        out_shape=(
            jax.ShapeDtypeStruct((1, pairs), F32),
            jax.ShapeDtypeStruct(response_queries.shape, BF16),
            jax.ShapeDtypeStruct(resp_kv.shape, BF16),
            jax.ShapeDtypeStruct(prompt_kv.shape, BF16),
        ),
        in_specs=[vmem] * 5,
        out_specs=(any_space,) * 4,
        scratch_shapes=[
            pltpu.VMEM((1, pairs), F32),
            pltpu.VMEM((slots, tokens, qw), BF16),
            pltpu.VMEM((slots, tokens, width), BF16),
            pltpu.VMEM(prompt_kv.shape, BF16),
            dma((3 * slots + 2,)),
        ],
        compiler_params=pltpu.CompilerParams(vmem_limit_bytes=16 * 1024 * 1024),
    )(*partial_outs)
    return margins.reshape(pairs), gq, gkv, gp


def solution(mesh):
    both = ("prefix", "resp")
    in_specs = (
        P(None, "prefix", None),
        P(both, None, None),
        P(both, None, None),
        P(both, None, None),
        P(both),
        P(),
        P(),
        P(),
    )
    out_specs = (
        P(),
        P(both, None, None),
        P(both, None, None),
        P(None, "prefix", None),
    )
    return jax.shard_map(
        functools.partial(on_device, mesh.shape["prefix"], mesh.shape["resp"]),
        mesh=mesh, in_specs=in_specs, out_specs=out_specs, check_vma=False,
    )
```

```python
import functools

import jax
import jax.numpy as jnp
from jax import lax
from jax.experimental import pallas as pl
from jax.experimental.pallas import tpu as pltpu
from jax.sharding import PartitionSpec as P

QUERY_HEADS = 14
KEY_VALUE_HEADS = 2
HEAD_SIZE = 128
LANES = 128
ROWS = 16

margin_beta = 0.1
loss_scale = 256.0
MESH = pl.DeviceIdType.MESH
F32 = jnp.float32
BF16 = jnp.bfloat16


def dot_nt(a, b):
    return lax.dot_general(a, b, (((1,), (1,)), ((), ())), preferred_element_type=F32)


def dot_nn(a, b):
    return lax.dot_general(a, b, (((1,), (0,)), ((), ())), preferred_element_type=F32)


def kernel(
    np_, nr,
    prompt_hbm, q_hbm, kv_hbm, ro_hbm, slot_hbm, len_hbm, pp_hbm, ppv_hbm, rm_hbm,
    margins_out, gq_s, gkv_s, fin_out, coef_out,
    full, qv, kvv, rov, slot_ref, len_ref, pp_ref, ppv_ref, rm_ref, ds_s, p_s, g_send, g_all, info_all, fin_all, lanes_s,
    in_sem, pk_ssem, pk_rsem, pd_ssem, pd_rsem, g_ssem, g_rsem, i_ssem, i_rsem, f_ssem, f_rsem,
):
    n = np_ * nr
    prompts, local, width = prompt_hbm.shape
    slots, tokens, _ = q_hbm.shape
    pairs = rm_hbm.shape[1]
    pl_w = info_all.shape[2]
    groups = QUERY_HEADS // KEY_VALUE_HEADS
    col_tiles = width // LANES
    tiles = (local // ROWS) * col_tiles
    total_len = full.shape[1]
    scale = HEAD_SIZE ** (-0.5)
    p = lax.axis_index("prefix")
    r = lax.axis_index("resp")
    me = p * nr + r

    def at_offset(k):
        other = lax.rem(me + k, n)
        return other, other // nr, lax.rem(other, nr)

    own_rows = full.at[:, pl.ds(pl.multiple_of(p * local, local), local), :]
    loads = [
        pltpu.make_async_copy(prompt_hbm, own_rows, in_sem.at[0]),
        pltpu.make_async_copy(q_hbm, qv, in_sem.at[1]),
        pltpu.make_async_copy(kv_hbm, kvv, in_sem.at[2]),
        pltpu.make_async_copy(ro_hbm, rov, in_sem.at[3]),
        pltpu.make_async_copy(slot_hbm, slot_ref, in_sem.at[4]),
        pltpu.make_async_copy(len_hbm, len_ref, in_sem.at[5]),
        pltpu.make_async_copy(pp_hbm, pp_ref, in_sem.at[6]),
        pltpu.make_async_copy(ppv_hbm, ppv_ref, in_sem.at[7]),
        pltpu.make_async_copy(rm_hbm, rm_ref, in_sem.at[8]),
    ]
    for c in loads:
        c.start()

    barrier = pltpu.get_barrier_semaphore()

    def greet(k, carry):
        _, op, orr = at_offset(k)
        pl.semaphore_signal(barrier, inc=1, device_id=(op, orr), device_id_type=MESH)
        return carry

    lax.fori_loop(1, n, greet, 0)

    lanes_s[...] = jnp.zeros_like(lanes_s)
    info_all[me] = jnp.zeros((info_all.shape[1], pl_w), F32)

    loads[0].wait()
    pl.semaphore_wait(barrier, n - 1)

    half = lax.rem(r, 2)
    partner = r + 1 - 2 * half
    half_width = width // 2

    def half_of(owner, which):
        rows = pl.ds(pl.multiple_of(owner * local, local), local)
        return full.at[:, rows, pl.ds(pl.multiple_of(which * half_width, half_width), half_width)]

    def prompt_copy(owner, to):
        part = half_of(owner, half)
        return pltpu.make_async_remote_copy(
            src_ref=part, dst_ref=part, send_sem=pk_ssem.at[to], recv_sem=pk_rsem.at[owner],
            device_id=(to, r), device_id_type=MESH,
        )

    def pass_copy(owner, which):
        part = half_of(owner, which)
        return pltpu.make_async_remote_copy(
            src_ref=part, dst_ref=part, send_sem=pd_ssem.at[owner], recv_sem=pd_rsem.at[owner],
            device_id=(p, partner), device_id_type=MESH,
        )

    others = [lax.rem(p + k, np_) for k in range(1, np_)]
    for o in others:
        prompt_copy(p, o).start()
    for c in loads[1:]:
        c.wait()
    lanes_s[0:1, 0:pairs] = rm_ref[...]
    lanes_s[1:2, 0:pairs] = ppv_ref[...].astype(F32)
    for o in others:
        prompt_copy(o, p).wait_recv()
        pass_copy(o, half).start()
    for o in others:
        pass_copy(o, 1 - half).wait_recv()

    causal = (
        lax.broadcasted_iota(jnp.int32, (tokens, tokens), 0)
        <= lax.broadcasted_iota(jnp.int32, (tokens, tokens), 1)
    )
    lane_t = lax.broadcasted_iota(jnp.int32, (1, tokens), 1)
    lane_k = lax.broadcasted_iota(jnp.int32, (1, pl_w), 1)

    def info_copy(sender, other, op, orr):
        return pltpu.make_async_remote_copy(
            src_ref=info_all.at[sender], dst_ref=info_all.at[sender],
            send_sem=i_ssem.at[other], recv_sem=i_rsem.at[sender],
            device_id=(op, orr), device_id_type=MESH,
        )

    def tile_copy(s, sender, other, op, orr):
        return pltpu.make_async_remote_copy(
            src_ref=g_send.at[s, op * tiles + orr], dst_ref=g_all.at[sender, s],
            send_sem=g_ssem.at[s, other], recv_sem=g_rsem.at[s, sender],
            device_id=(op, orr), device_id_type=MESH,
        )

    def when_owner(rank, f):
        if nr == tiles:
            f()
        else:
            pl.when(rank < tiles)(f)

    def one_slot(s, carry):
        response = slot_ref[s]
        pair = lax.shift_right_logical(response, 1)
        sign = 1.0 - 2.0 * lax.bitwise_and(response, 1).astype(F32)
        valid = (lane_t < len_ref[response]).astype(F32)
        a = pp_ref[pair]
        logp = jnp.zeros((1, tokens), F32)
        for g in range(KEY_VALUE_HEADS):
            kc = slice(g * HEAD_SIZE, (g + 1) * HEAD_SIZE)
            vc = slice((KEY_VALUE_HEADS + g) * HEAD_SIZE, (KEY_VALUE_HEADS + g + 1) * HEAD_SIZE)
            keys = jnp.concatenate([full[a, :, kc], kvv[s, :, kc]], axis=0)
            values = jnp.concatenate([full[a, :, vc], kvv[s, :, vc]], axis=0)
            for j in range(groups):
                h = g * groups + j
                hc = slice(h * HEAD_SIZE, (h + 1) * HEAD_SIZE)
                jc = slice(j * tokens, (j + 1) * tokens)
                sc = dot_nt(keys, qv[s, :, hc])
                dp = dot_nt(values, rov[s, :, hc])
                sp = sc[:total_len]
                so = jnp.where(causal, sc[total_len:], -jnp.inf)
                top = jnp.maximum(
                    jnp.max(sp, axis=0, keepdims=True), jnp.max(so, axis=0, keepdims=True)
                )
                sc = jnp.concatenate([sp, so], axis=0)
                e = jnp.exp((sc - top) * scale)
                inv = valid / jnp.sum(e, axis=0, keepdims=True)
                pb = (e * inv).astype(BF16)
                pf = pb.astype(F32)
                delta = jnp.sum(pf * dp, axis=0, keepdims=True)
                logp = logp + delta
                p_s[:, jc] = pb
                ds_s[:, jc] = (pf * (dp - delta)).astype(BF16)
            gqt = dot_nn(keys.T, ds_s[...])
            for j in range(groups):
                h = g * groups + j
                hc = slice(h * HEAD_SIZE, (h + 1) * HEAD_SIZE)
                gq_s[s, :, hc] = gqt[:, j * tokens:(j + 1) * tokens].T.astype(BF16)
            heads = range(g * groups, (g + 1) * groups)
            qs = jnp.concatenate([qv[s, :, h * HEAD_SIZE:(h + 1) * HEAD_SIZE] for h in heads], axis=0)
            rs = jnp.concatenate([rov[s, :, h * HEAD_SIZE:(h + 1) * HEAD_SIZE] for h in heads], axis=0)
            gk = dot_nn(ds_s[...], qs) * scale
            gv = dot_nn(p_s[...], rs)
            gkv_s[s, :, kc] = gk[total_len:]
            gkv_s[s, :, vc] = gv[total_len:]
            for o in range(np_):
                for i in range(local // ROWS):
                    rows = slice(o * local + i * ROWS, o * local + (i + 1) * ROWS)
                    at = o * tiles + i * col_tiles
                    g_send[s, at + g] = gk[rows].astype(BF16)
                    g_send[s, at + KEY_VALUE_HEADS + g] = gv[rows].astype(BF16)
        hot = jnp.where(lane_k == pair, sign, 0.0)
        info_all[me, pl.ds(s, 1), :] = hot
        info_all[me, pl.ds(slots + s, 1), :] = hot * jnp.sum(logp, axis=1, keepdims=True)

        def send_tile(k, c):
            other, op, orr = at_offset(k)
            when_owner(orr, lambda: tile_copy(s, me, other, op, orr).start())
            return c

        lax.fori_loop(1, n, send_tile, 0)
        return carry

    lax.fori_loop(0, slots, one_slot, 0)

    def send(k, carry):
        other, op, orr = at_offset(k)
        info_copy(me, other, op, orr).start()
        return carry

    lax.fori_loop(1, n, send, 0)

    def take_own():
        for s in range(slots):
            g_all[me, s] = g_send[s, p * tiles + r]

    when_owner(r, take_own)

    def info_wait(k, carry):
        other, op, orr = at_offset(k)
        info_copy(other, other, op, orr).wait_recv()
        return carry

    lax.fori_loop(1, n, info_wait, 0)

    chunk = min(n, 32)

    def add_info(c, acc):
        return acc + jnp.sum(info_all[pl.ds(c * chunk, chunk)], axis=0)

    sums = lax.fori_loop(0, n // chunk, add_info, jnp.zeros((info_all.shape[1], pl_w), F32))
    pair_sums = jnp.sum(sums[slots:2 * slots], axis=0, keepdims=True)
    margins = margin_beta * (pair_sums - lanes_s[0:1, :])
    margins_out[...] = margins[:, 0:pairs]
    weights = -loss_scale * margin_beta * jax.nn.sigmoid(-margins)
    weights = jnp.where(lane_k < pairs, weights, 0.0)
    for s in range(slots):
        coef = jnp.sum(info_all[me, s:s + 1, :] * weights, axis=1, keepdims=True)
        coef_out[s:s + 1, :] = jnp.broadcast_to(coef, (1, LANES))

    def finish_tile():
        def tile_wait(k, carry):
            other, op, orr = at_offset(k)
            for s in range(slots):
                pltpu.make_async_remote_copy(
                    src_ref=g_send.at[s, 0], dst_ref=g_all.at[other, s],
                    send_sem=g_ssem.at[s, other], recv_sem=g_rsem.at[s, other],
                    device_id=(op, orr), device_id_type=MESH,
                ).wait_recv()
            return carry

        lax.fori_loop(1, n, tile_wait, 0)

        def add_tiles(c, acc):
            x = info_all[pl.ds(c * chunk, chunk)]
            acc = list(acc)
            for a in range(prompts):
                wa = jnp.where(lanes_s[1:2, :] == float(a), weights, 0.0)
                ca = jnp.sum(x * wa[None], axis=-1, keepdims=True)
                for d in range(chunk):
                    for s in range(slots):
                        acc[a] = acc[a] + ca[d, s:s + 1, :] * g_all[c * chunk + d, s].astype(F32)
            return tuple(acc)

        zero = tuple(jnp.zeros((ROWS, LANES), F32) for _ in range(prompts))
        acc = lax.fori_loop(0, n // chunk, add_tiles, zero)
        for a in range(prompts):
            fin_all[r, a] = acc[a].astype(BF16)

        def fin_send(k, carry):
            orr = lax.rem(r + k, nr)
            pltpu.make_async_remote_copy(
                src_ref=fin_all.at[r], dst_ref=fin_all.at[r],
                send_sem=f_ssem.at[orr], recv_sem=f_rsem.at[r],
                device_id=(p, orr), device_id_type=MESH,
            ).start()
            return carry

        lax.fori_loop(1, nr, fin_send, 0)

    when_owner(r, finish_tile)

    def fin_copy(sender, other):
        return pltpu.make_async_remote_copy(
            src_ref=fin_all.at[sender], dst_ref=fin_all.at[sender],
            send_sem=f_ssem.at[other], recv_sem=f_rsem.at[sender],
            device_id=(p, other), device_id_type=MESH,
        )

    def fin_wait(k, carry):
        other = lax.rem(r + k, nr)
        when_owner(other, lambda: fin_copy(other, other).wait_recv())
        return carry

    lax.fori_loop(1, nr, fin_wait, 0)
    fin_out[...] = fin_all[...]

    def drain(k, carry):
        other, op, orr = at_offset(k)
        info_copy(me, other, op, orr).wait_send()
        for s in range(slots):
            when_owner(orr, lambda s=s: tile_copy(s, me, other, op, orr).wait_send())
        return carry

    lax.fori_loop(1, n, drain, 0)
    for o in others:
        prompt_copy(p, o).wait_send()
        pass_copy(o, half).wait_send()

    def drain_fin():
        def one(k, carry):
            fin_copy(r, lax.rem(r + k, nr)).wait_send()
            return carry

        lax.fori_loop(1, nr, one, 0)

    when_owner(r, drain_fin)


def finish(margins_ref, gq_ref, gkv_ref, fin_ref, coef_ref, margins_out, gq_out, gkv_out, gp_out, mv, qv, kvv, gpv, sems):
    slots, tokens, qw = gq_ref.shape
    tiles, prompts, _, _ = fin_ref.shape
    width = gkv_ref.shape[2]
    col_tiles = width // LANES
    scale = HEAD_SIZE ** (-0.5)
    pieces = 2
    step = tokens // pieces
    copies = []

    def put(src, dst):
        c = pltpu.make_async_copy(src, dst, sems.at[len(copies)])
        c.start()
        copies.append(c)

    for s in range(slots):
        coef = coef_ref[s:s + 1, 0:1]
        for t in range(pieces):
            rows = slice(t * step, (t + 1) * step)
            qv[s, rows] = (gq_ref[s, rows].astype(F32) * (coef * scale)).astype(BF16)
            put(qv.at[s, rows], gq_out.at[s, rows])
        kvv[s] = (gkv_ref[s] * coef).astype(BF16)
        put(kvv.at[s], gkv_out.at[s])
    for t in range(tiles):
        i, j = divmod(t, col_tiles)
        for a in range(prompts):
            gpv[a, i * ROWS:(i + 1) * ROWS, j * LANES:(j + 1) * LANES] = fin_ref[t, a]
    put(gpv, gp_out)
    mv[...] = margins_ref[...]
    put(mv, margins_out)
    for c in copies:
        c.wait()


def on_device(np_, nr, prompt_kv, response_queries, resp_kv, readout, slot_response, lengths, pair_prompt, ref_margin):
    n = np_ * nr
    prompts, local, width = prompt_kv.shape
    slots, tokens, qw = response_queries.shape
    pairs = ref_margin.shape[0]
    pl_w = -(-pairs // LANES) * LANES
    total_len = local * np_
    groups = QUERY_HEADS // KEY_VALUE_HEADS
    tiles = (local // ROWS) * (width // LANES)
    assert nr >= tiles
    info_rows = 2 * slots
    assert nr % 2 == 0
    keys = total_len + tokens
    hbm = pl.BlockSpec(memory_space=pltpu.HBM)
    vmem = pl.BlockSpec(memory_space=pltpu.VMEM)
    dma = pltpu.SemaphoreType.DMA
    partial_outs = pl.pallas_call(
        functools.partial(kernel, np_, nr),
        name="dpo_attention",
        out_shape=(
            jax.ShapeDtypeStruct((1, pairs), F32),
            jax.ShapeDtypeStruct(response_queries.shape, BF16),
            jax.ShapeDtypeStruct(resp_kv.shape, F32),
            jax.ShapeDtypeStruct((tiles, prompts, ROWS, LANES), BF16),
            jax.ShapeDtypeStruct((8, LANES), F32),
        ),
        in_specs=[hbm] * 9,
        out_specs=(vmem,) * 5,
        scratch_shapes=[
            pltpu.VMEM((prompts, total_len, width), BF16),
            pltpu.VMEM((slots, tokens, qw), BF16),
            pltpu.VMEM((slots, tokens, width), BF16),
            pltpu.VMEM((slots, tokens, qw), BF16),
            pltpu.SMEM(slot_response.shape, jnp.int32),
            pltpu.SMEM(lengths.shape, jnp.int32),
            pltpu.SMEM(pair_prompt.shape, jnp.int32),
            pltpu.VMEM((1, pairs), jnp.int32),
            pltpu.VMEM((1, pairs), F32),
            pltpu.VMEM((keys, groups * tokens), BF16),
            pltpu.VMEM((keys, groups * tokens), BF16),
            pltpu.VMEM((slots, np_ * tiles, ROWS, LANES), BF16),
            pltpu.VMEM((n, slots, ROWS, LANES), BF16),
            pltpu.VMEM((n, info_rows, pl_w), F32),
            pltpu.VMEM((tiles, prompts, ROWS, LANES), BF16),
            pltpu.VMEM((8, pl_w), F32),
            dma((9,)),
            dma((np_,)), dma((np_,)), dma((np_,)), dma((np_,)),
            dma((slots, n)), dma((slots, n)),
            dma((n,)), dma((n,)),
            dma((nr,)), dma((nr,)),
        ],
        compiler_params=pltpu.CompilerParams(
            collective_id=0, has_side_effects=True
        ),
    )(
        prompt_kv, response_queries, resp_kv, readout, slot_response, lengths, pair_prompt,
        pair_prompt.reshape(1, pairs), ref_margin.reshape(1, pairs),
    )
    margins, gq, gkv, gp = pl.pallas_call(
        finish,
        name="scale_and_store",
        out_shape=(
            jax.ShapeDtypeStruct((1, pairs), F32),
            jax.ShapeDtypeStruct(response_queries.shape, BF16),
            jax.ShapeDtypeStruct(resp_kv.shape, BF16),
            jax.ShapeDtypeStruct(prompt_kv.shape, BF16),
        ),
        in_specs=[vmem] * 5,
        out_specs=(hbm,) * 4,
        scratch_shapes=[
            pltpu.VMEM((1, pairs), F32),
            pltpu.VMEM((slots, tokens, qw), BF16),
            pltpu.VMEM((slots, tokens, width), BF16),
            pltpu.VMEM(prompt_kv.shape, BF16),
            dma((3 * slots + 2,)),
        ],
    )(*partial_outs)
    return margins.reshape(pairs), gq, gkv, gp


def solution(mesh):
    both = ("prefix", "resp")
    in_specs = (
        P(None, "prefix", None),
        P(both, None, None),
        P(both, None, None),
        P(both, None, None),
        P(both),
        P(),
        P(),
        P(),
    )
    out_specs = (
        P(),
        P(both, None, None),
        P(both, None, None),
        P(None, "prefix", None),
    )
    return jax.shard_map(
        functools.partial(on_device, mesh.shape["prefix"], mesh.shape["resp"]),
        mesh=mesh, in_specs=in_specs, out_specs=out_specs, check_vma=False,
    )
```
